256 devices in a mesh: tok: 8 (over z_hi, x), head: 32 (over y, z_lo, core).
Axes of the slice: x: 4, y: 4, z: 8 (z_hi: 2, z_lo: 4; z = z_hi * 4 + z_lo), core: 2. Of those that a mesh axis runs over, the one named last changes fastest.
Arguments:
- query_states: bfloat16 [16384, 8192], P(('tok', 'head')), may hold values from -7.5 to 7.5
- key_states: bfloat16 [16384, 8192], P(('tok', 'head')), may hold values from -7.5 to 7.5
- value_states: bfloat16 [16384, 8192], P(('tok', 'head')), may hold values from -6 to 6
- token_rates: float32 [32, 16384], P('head', 'tok'), may hold values from 0.05 to 1
- fast_weights: bfloat16 [32, 512, 768], P('head'), may hold values from -0.375 to 0.375
Outputs:
- combined: bfloat16 [16384, 8192], P(('tok', 'head'))
- new_weights: bfloat16 [32, 512, 768], P('head', 'tok')
The draws below stay inside these ranges and needn't reach their ends.
All inputs are finite; a program needn't handle non-finite values.
Results may differ from the reference program's by a relative error of at most 0.039.
Values may be sent and summed in bfloat16 or wider, within the bound.
No kernel may reach another device: no remote copies, remote signals or barrier semaphores. Data moves between devices by JAX's collectives and lax.ppermute only.
A program may use at most 64 MiB of HBM per device.

```python
import math
import jax
import jax.numpy as jnp
from jax import lax

DH = 256
FH = 512
WINDOW = 1024
NS_STEPS = 5
TOK_DEV = 2048
HEADS = 32
D = 8192
TOKENS = 16384


def draw_query_states(key, part):
    own_key = jax.random.fold_in(key, 1)
    states = jnp.clip(jax.random.normal(own_key, (TOKENS, D), jnp.float32), -6.0, 6.0)
    return states.astype(jnp.bfloat16)


def draw_key_states(key, part):
    own_key = jax.random.fold_in(key, 2)
    states = jnp.clip(jax.random.normal(own_key, (TOKENS, D), jnp.float32), -6.0, 6.0)
    return states.astype(jnp.bfloat16)


def steps_of(key, shape, shards, smallest, largest):
    level = 1.0
    for dim, shards_of in shards:
        draws = jax.random.uniform(jax.random.fold_in(jax.random.fold_in(key, 6), dim), (shards_of,), jnp.float32, smallest / len(shards), largest / len(shards))
        level = level * jnp.repeat(jnp.exp(draws), shape[dim] // shards_of).reshape((-1,) + (1,) * (len(shape) - 1 - dim))
    return level


def scatter_about(rng, extent, deviation, most, split=(), kind=jnp.bfloat16):
    entries = jax.random.normal(rng, extent, jnp.float32) * deviation
    if len(split) > 0:
        entries = steps_of(rng, extent, split, -0.22, 0.18) * entries
    return jnp.clip(entries, min=-most, max=most).astype(kind)


def setup_inputs(seed: int = 0) -> dict:
    streams_of = jax.random.split(jax.random.key(seed), 6)
    query_states = draw_query_states(jax.random.fold_in(streams_of[5], 71), 0)
    key_states = draw_key_states(jax.random.fold_in(streams_of[5], 71), 0)
    value_states = scatter_about(streams_of[2], (TOKENS, D), 1.0, 6.0, ((0, 256),))
    token_rates = jnp.clip(jnp.exp(math.log(1.0) - 2.9957323 * jax.random.uniform(streams_of[3], (HEADS, TOKENS), jnp.float32) ** steps_of(streams_of[3], (HEADS, TOKENS), ((0, 32), (1, 8)), -0.2, 0.2)), 0.05, 1.0)
    fast_weights = scatter_about(streams_of[4], (HEADS, FH, 3 * DH), DH ** -0.5, 0.375, ((0, 32),))
    return {"query_states": query_states, "key_states": key_states, "value_states": value_states, "token_rates": token_rates, "fast_weights": fast_weights}


coef_linear = 3.4445
coef_cubic = -4.775
coef_quintic = 2.0315
epsilon = 1e-06

def block_size(local_rows):
    return 512 if local_rows % 512 == 0 else local_rows

def rms_norm(values):
    return values * lax.rsqrt(lax.optimization_barrier(jnp.mean(values * values, axis=-1, keepdims=True)) + epsilon)

def silu_parts(gate_value):
    sigmoid = jax.nn.sigmoid(gate_value)
    return (gate_value * sigmoid, sigmoid * (1.0 + gate_value * (1.0 - sigmoid)))

def project(inputs, weights):
    gate_value = jnp.dot(inputs, weights[:, :DH].T, preferred_element_type=jnp.float32)
    up_value = jnp.dot(inputs, weights[:, DH:2 * DH].T, preferred_element_type=jnp.float32)
    return (gate_value, up_value)

def attend(query_rows, key_rows, value_rows, positions, key_positions):
    scores = jnp.dot(query_rows, key_rows.T, preferred_element_type=jnp.float32) * DH ** (-0.5)
    offset = positions[:, None] - key_positions[None, :]
    allowed = (offset >= 0) & (offset < WINDOW) & (key_positions[None, :] >= 0)
    scores = jnp.where(allowed, scores, -1e+30)
    highest = lax.optimization_barrier(jnp.max(scores, axis=1, keepdims=True))
    expo = jnp.exp(scores - highest)
    probs = (expo / lax.optimization_barrier(jnp.sum(expo, axis=1, keepdims=True))).astype(jnp.bfloat16)
    return jnp.dot(probs, value_rows, preferred_element_type=jnp.float32)

def attention_head(query_rows, key_rows, value_rows):
    block_rows = block_size(TOK_DEV)
    padded_keys = jnp.concatenate([jnp.zeros((WINDOW, DH), jnp.bfloat16), key_rows])
    padded_values = jnp.concatenate([jnp.zeros((WINDOW, DH), jnp.bfloat16), value_rows])

    def attend_block(block_index):
        offset = (block_index * block_rows).astype(jnp.int32)
        queries_here = lax.dynamic_slice_in_dim(query_rows, offset, block_rows, 0)
        keys_here = lax.dynamic_slice_in_dim(padded_keys, offset, block_rows + WINDOW, 0)
        values_here = lax.dynamic_slice_in_dim(padded_values, offset, block_rows + WINDOW, 0)
        positions = offset + jnp.arange(block_rows).astype(jnp.int32)
        key_positions = offset - WINDOW + jnp.arange(block_rows + WINDOW).astype(jnp.int32)
        return attend(queries_here, keys_here, values_here, positions, key_positions)
    blocks = lax.map(attend_block, jnp.arange(TOKENS // block_rows).astype(jnp.int32))
    return blocks.reshape(TOKENS, DH)

def newton_schulz(gradient):
    squares = lax.optimization_barrier(jnp.sum(gradient * gradient, axis=(0, 2)))
    iterate = (gradient * lax.rsqrt(squares + epsilon)[None, :, None]).astype(jnp.bfloat16)
    for repeat_index in range(NS_STEPS):
        wide = iterate.astype(jnp.float32)
        gram_matrix = jnp.einsum('fjd,fje->jde', wide, wide, precision=lax.Precision.HIGHEST).astype(jnp.bfloat16)
        gram_wide = gram_matrix.astype(jnp.float32)
        square_gram = jnp.einsum('jde,jef->jdf', gram_wide, gram_wide, precision=lax.Precision.HIGHEST)
        polynomial = (coef_cubic * gram_wide + coef_quintic * square_gram).astype(jnp.bfloat16)
        iterate = (coef_linear * wide + jnp.einsum('fjd,jde->fje', wide, polynomial.astype(jnp.float32), precision=lax.Precision.HIGHEST)).astype(jnp.bfloat16)
    return iterate

def fast_head(query_rows, key_rows, value_rows, rate_rows, weights):
    gate_value, up_value = project(key_rows, weights)
    gate_silu, gate_slope = silu_parts(gate_value)
    hidden = (gate_silu * up_value).astype(jnp.bfloat16)
    target = (-rate_rows[:, None] * value_rows.astype(jnp.float32)).astype(jnp.bfloat16)
    back_grad = jnp.dot(target, weights[:, 2 * DH:].T, preferred_element_type=jnp.float32)
    gate_grad = (back_grad * up_value * gate_slope).astype(jnp.bfloat16)
    up_grad = (back_grad * gate_silu).astype(jnp.bfloat16)
    gradient = jnp.concatenate([jnp.dot(gate_grad.T, key_rows, preferred_element_type=jnp.float32), jnp.dot(up_grad.T, key_rows, preferred_element_type=jnp.float32), jnp.dot(hidden.T, target, preferred_element_type=jnp.float32)], axis=1)
    iterate = newton_schulz(gradient.reshape(FH, 3, DH))
    updated = (weights.reshape(FH, 3, DH).astype(jnp.float32) - iterate.astype(jnp.float32)).astype(jnp.bfloat16).reshape(FH, 3 * DH)
    query_gate, query_up = project(query_rows, updated)
    query_hidden = (jax.nn.silu(query_gate) * query_up).astype(jnp.bfloat16)
    applied = jnp.dot(query_hidden, updated[:, 2 * DH:], preferred_element_type=jnp.float32)
    return (rms_norm(applied), updated)

def reference(query_states, key_states, value_states, token_rates, fast_weights):

    def split_heads(states):
        return states.reshape(TOKENS, HEADS, DH).transpose(1, 0, 2)

    def per_head(items):
        query_rows, key_rows, value_rows, rate_rows, weights = items
        attended = rms_norm(attention_head(query_rows, key_rows, value_rows))
        applied, updated = fast_head(query_rows, key_rows, value_rows, rate_rows, weights)
        return ((attended + applied).astype(jnp.bfloat16), updated)
    combined, new_weights = lax.map(per_head, (split_heads(query_states), split_heads(key_states), split_heads(value_states), token_rates, fast_weights))
    return (combined.transpose(1, 0, 2).reshape(TOKENS, D), new_weights)
```

```python
import functools

import jax
import jax.numpy as jnp
from jax import lax
from jax.experimental import pallas as pl
from jax.experimental.pallas import tpu as pltpu
from jax.sharding import Mesh
from jax.sharding import PartitionSpec as P

DH = 256
FH = 512
WINDOW = 1024
NS_STEPS = 5
TOK = ("tok_0", "tok_1")
TOK_HEAD = ("tok_0", "tok_1", "head")
RING = 4
PIECE = 3 * DH // RING

coef_linear = 3.4445
coef_cubic = -4.775
coef_quintic = 2.0315
epsilon = 1e-06

F32 = jnp.float32
BF16 = jnp.bfloat16
LOG2E = 1.4426950408889634
SCALE2 = DH ** (-0.5) * LOG2E


def mm_nt(a, b):
    return lax.dot_general(a, b, (((1,), (1,)), ((), ())), preferred_element_type=F32)


def mm_tn(a, b):
    return lax.dot_general(a, b, (((0,), (0,)), ((), ())), preferred_element_type=F32)


def mm(a, b):
    return jnp.dot(a, b, preferred_element_type=F32)


def sigmoid(x):
    return 0.5 * jnp.tanh(0.5 * x) + 0.5


def rms_norm(values):
    return values * lax.rsqrt(jnp.mean(values * values, axis=-1, keepdims=True) + epsilon)


def gradient_kernel(index_ref, kv_ref, w_ref, r_ref, own_ref, s1_ref, s2_ref, s3_ref, acc_ref):
    rates = r_ref[...].T
    chunk = 8
    rows = chunk * 64
    for c in range(32 // chunk):
        keys = kv_ref[c * chunk : (c + 1) * chunk, 0:64, :].reshape(rows, DH)
        values = kv_ref[c * chunk : (c + 1) * chunk, 64:128, :].reshape(rows, DH).astype(F32)
        groups = rows // 128
        target = jnp.concatenate(
            [
                (-rates[:, groups * c + j : groups * c + j + 1] * values[j * 128 : (j + 1) * 128])
                for j in range(groups)
            ],
            axis=0,
        ).astype(BF16)
        gate = mm_nt(keys, w_ref[:, 0:DH])
        up = mm_nt(keys, w_ref[:, DH : 2 * DH])
        back = mm_nt(target, w_ref[:, 2 * DH : 3 * DH])
        s = sigmoid(gate)
        silu = gate * s
        hidden = (silu * up).astype(BF16)
        gate_grad = (back * up * (s * (1.0 + gate * (1.0 - s)))).astype(BF16)
        up_grad = (back * silu).astype(BF16)
        parts = (mm_tn(keys, gate_grad), mm_tn(keys, up_grad), mm_tn(target, hidden))
        for b in range(3):
            if c == 0:
                acc_ref[b * DH : (b + 1) * DH, :] = parts[b]
            else:
                acc_ref[b * DH : (b + 1) * DH, :] += parts[b]
    x = index_ref[1]
    for d, ref in enumerate((own_ref, s1_ref, s2_ref, s3_ref)):
        start = pl.multiple_of(((x + d) & (RING - 1)) * PIECE, PIECE)
        ref[...] = acc_ref[pl.ds(start, PIECE), :].astype(ref.dtype)


def gradient_pieces(index, kv, weights, rates):
    vmem = pl.BlockSpec(memory_space=pltpu.VMEM)
    piece = jax.ShapeDtypeStruct((PIECE, FH), BF16)
    return pl.pallas_call(
        gradient_kernel,
        in_specs=[pl.BlockSpec(memory_space=pltpu.SMEM), vmem, vmem, vmem],
        out_specs=[vmem] * 4,
        out_shape=[jax.ShapeDtypeStruct((PIECE, FH), F32), piece, piece, piece],
        scratch_shapes=[pltpu.VMEM((3 * DH, FH), F32)],
        compiler_params=pltpu.CompilerParams(vmem_limit_bytes=40 * 2**20),
        cost_estimate=pl.CostEstimate(flops=6 * 2 * 2048 * DH * FH, bytes_accessed=4 * 2**20, transcendentals=2**20),
        name="gradient",
    )(index, kv, weights, rates)


def attention_kernel(index_ref, q_ref, prev_ref, own_ref, out_ref, *, check):
    row = lax.broadcasted_iota(jnp.int32, (DH, DH), 0)
    col = lax.broadcasted_iota(jnp.int32, (DH, DH), 1)
    bias = jnp.where(index_ref[0] > 0, 0.0, -1e30).astype(F32)

    def piece(j, lo):
        ref, at = (prev_ref, 4 * j) if j < 4 else (own_ref, 4 * (j - 4))
        return ref[at : at + 4, lo : lo + 64, :].reshape(256, DH)

    for b in range(4):
        queries = q_ref[4 * b : 4 * b + 4].reshape(256, DH)
        scores = []
        for j in range(5):
            s = mm_nt(queries, piece(b + j, 0))
            if check and b + j < 4:
                s = s + bias
            if j == 0:
                s = jnp.where(col > row, s, -1e30)
            if j == 4:
                s = jnp.where(col <= row, s, -1e30)
            scores.append(s)
        top = functools.reduce(jnp.maximum, scores)
        highest = jnp.max(top, axis=1, keepdims=True)
        expo = [jnp.exp2((s - highest) * SCALE2) for s in scores]
        total = jnp.sum(functools.reduce(jnp.add, expo), axis=1, keepdims=True)
        probs = jnp.concatenate([e.astype(BF16) for e in expo], axis=1)
        values = jnp.concatenate([piece(b + j, 64) for j in range(5)], axis=0)
        out_ref[b * 256 : (b + 1) * 256, :] = rms_norm(mm(probs, values) / total)


def attention(index, query_rows, half, prev, prev_block, own, own_block, check):
    def whole(block):
        return lambda step: (block, 0, 0)

    return pl.pallas_call(
        functools.partial(attention_kernel, check=check),
        grid=(1,),
        in_specs=[
            pl.BlockSpec(memory_space=pltpu.SMEM),
            pl.BlockSpec((16, 64, DH), whole(half)),
            pl.BlockSpec((16, 128, DH), whole(prev_block)),
            pl.BlockSpec((16, 128, DH), whole(own_block)),
        ],
        out_specs=pl.BlockSpec((1024, DH), lambda step: (0, 0)),
        out_shape=jax.ShapeDtypeStruct((1024, DH), F32),
        compiler_params=pltpu.CompilerParams(vmem_limit_bytes=40 * 2**20),
        cost_estimate=pl.CostEstimate(flops=4 * 1024 * 1280 * DH, bytes_accessed=4 * 2**20, transcendentals=1024 * 1280),
        name="attention",
    )(index, query_rows, prev, own)


def update_kernel(index_ref, p0_ref, p1_ref, p2_ref, p3_ref, w_ref, q_ref, first_ref, second_ref, out_ref, nw_ref, y_ref, w2_ref):
    x = index_ref[1]
    for d, ref in enumerate((p0_ref, p1_ref, p2_ref, p3_ref)):
        start = pl.multiple_of(((x + RING - d) & (RING - 1)) * PIECE, PIECE)
        y_ref[pl.ds(start, PIECE), :] = ref[...]
    iterates = []
    for b in range(3):
        g = y_ref[b * DH : (b + 1) * DH, :].astype(F32)
        iterates.append((g * lax.rsqrt(jnp.sum(g * g, keepdims=True) + epsilon)).astype(BF16))
    for step in range(NS_STEPS):
        grams = [mm_nt(y, y).astype(BF16) for y in iterates]
        squares = [mm(a, a) for a in grams]
        polys = [(coef_cubic * a.astype(F32) + coef_quintic * s).astype(BF16) for a, s in zip(grams, squares)]
        iterates = [(coef_linear * y.astype(F32) + mm(p, y)).astype(BF16) for p, y in zip(polys, iterates)]
    for b in range(3):
        block = w_ref[:, b * DH : (b + 1) * DH].astype(F32) - iterates[b].astype(F32).T
        w2_ref[:, b * DH : (b + 1) * DH] = block.astype(BF16)
    nw_ref[...] = w2_ref[pl.ds(pl.multiple_of(index_ref[0] * 64, 64), 64), :]
    chunk = 8
    rows = chunk * 64
    for c in range(32 // chunk):
        queries = q_ref[c * chunk : (c + 1) * chunk].reshape(rows, DH)
        gate = mm_nt(queries, w2_ref[:, 0:DH])
        up = mm_nt(queries, w2_ref[:, DH : 2 * DH])
        hidden = (gate * sigmoid(gate) * up).astype(BF16)
        applied = rms_norm(mm(hidden, w2_ref[:, 2 * DH : 3 * DH]))
        ref, at = (first_ref, c * rows) if c < 2 else (second_ref, (c - 2) * rows)
        out_ref[c * chunk : (c + 1) * chunk] = (ref[at : at + rows, :] + applied).astype(BF16).reshape(chunk, 64, DH)


def update_and_apply(index, pieces, weights, query_rows, first, second):
    vmem = pl.BlockSpec(memory_space=pltpu.VMEM)
    return pl.pallas_call(
        update_kernel,
        in_specs=[pl.BlockSpec(memory_space=pltpu.SMEM)] + [vmem] * 8,
        out_specs=[vmem, vmem],
        out_shape=[jax.ShapeDtypeStruct((32, 64, DH), BF16), jax.ShapeDtypeStruct((64, 3 * DH), BF16)],
        scratch_shapes=[pltpu.VMEM((3 * DH, FH), BF16), pltpu.VMEM((FH, 3 * DH), BF16)],
        compiler_params=pltpu.CompilerParams(vmem_limit_bytes=40 * 2**20),
        cost_estimate=pl.CostEstimate(flops=2**33, bytes_accessed=8 * 2**20, transcendentals=2**20),
        name="update",
    )(index, *pieces, weights, query_rows, first, second)


def by_head(states):
    return states.reshape(64, 32, DH).transpose(1, 0, 2)


def exchange(pieces):
    return lax.all_to_all(pieces, "head", split_axis=0, concat_axis=0, tiled=True)


def around(value, axis, steps):
    count = lax.axis_size(axis)
    return lax.ppermute(value, axis, [(k, (k + steps) % count) for k in range(count)])


def per_device(query_states, key_states, value_states, token_rates, fast_weights):
    kv = exchange(jnp.concatenate([by_head(key_states), by_head(value_states)], axis=1))
    query_states, kv = lax.optimization_barrier((query_states, kv))
    query_rows = exchange(by_head(query_states))
    tok_count = lax.axis_size(TOK)
    halo = lax.ppermute(kv[16:32], TOK, [(k, k + 1) for k in range(tok_count - 1)])
    index = jnp.stack([lax.axis_index(TOK), lax.axis_index("tok_1")]).astype(jnp.int32)
    weights = fast_weights[0]
    own, *sends = gradient_pieces(index, kv, weights, token_rates.reshape(16, 128))
    summed = own
    for d in range(1, RING):
        summed = summed + around(sends[d - 1], "tok_1", d).astype(F32)
    summed = summed.astype(BF16)
    other = around(summed, "tok_0", 1)
    summed = (summed.astype(F32) + other.astype(F32)).astype(BF16)
    pieces = [summed] + [around(summed, "tok_1", d) for d in range(1, RING)]
    second = attention(index, query_rows, 1, kv, 0, kv, 1, False)
    first = attention(index, query_rows, 0, halo, 0, kv, 0, True)
    combined, owned = update_and_apply(index, pieces, weights, query_rows, first, second)
    combined = exchange(combined).transpose(1, 0, 2).reshape(64, 32 * DH)
    return (combined, owned[None])


def solution(mesh):
    finer = Mesh(mesh.devices.reshape(2, RING, mesh.shape["head"]), ("tok_0", "tok_1", "head"))
    return jax.shard_map(
        per_device,
        mesh=finer,
        in_specs=(
            P(TOK_HEAD, None),
            P(TOK_HEAD, None),
            P(TOK_HEAD, None),
            P("head", TOK),
            P("head", None, None),
        ),
        out_specs=(P(TOK_HEAD, None), P("head", TOK, None)),
        check_vma=False,
    )
```
